128 devices in a mesh: row: 16 (over x, y_lo, core), col: 8 (over z, y_hi).
Axes of the slice: x: 4, y: 4 (y_hi: 2, y_lo: 2; y = y_hi * 2 + y_lo), z: 4, core: 2. Of those that a mesh axis runs over, the one named last changes fastest.
Arguments:
- upper_s: float32 [2, 4096, 4, 2048], P(None, 'row', None, 'col')
- upper_t: float32 [2, 4096, 4, 2048], P(None, 'row', None, 'col')
- left_vectors: float32 [2, 4096, 4, 2048], P(None, 'row', None, 'col'), may hold values from -6 to 6
- right_vectors: float32 [2, 4096, 4, 2048], P(None, 'row', None, 'col'), may hold values from -6 to 6
- window_starts: int32 [3, 16], replicated, may hold values from 0 to 31, as said below
- selection: int32 [3, 16, 256], replicated, may hold values 0 or 1
- window_factors: float32 [3, 16, 2, 256, 256], P(None, 'row')
Outputs:
- new_s: float32 [2, 4096, 4, 2048], P(None, 'row', None, 'col')
- new_t: float32 [2, 4096, 4, 2048], P(None, 'row', None, 'col')
- new_left: float32 [2, 4096, 4, 2048], P(None, 'row', None, 'col')
- new_right: float32 [2, 4096, 4, 2048], P(None, 'row', None, 'col')
The draws below stay inside these ranges and needn't reach their ends.
Inputs may be any that keep to these rules, and one draw needn't show every extreme that they name: `window_starts`: within each round the 16 block numbers are distinct.
All inputs are finite; a program needn't handle non-finite values.
Results may differ from the reference program's by a relative error of at most 0.0001.
Values sent between devices are 32-bit elements; how exact they have to be, the bound alone decides.
A program may use at most 128 MiB of HBM per device.

```python
import jax
import jax.numpy as jnp
from jax import lax

N = 8192
W = 256
NWIN = 16
ROUNDS = 3
BR = 2
BC = 4
N_ROW = 16
N_COL = 8


def draw_upper_s(key, part):
    values = jax.random.normal(jax.random.fold_in(key, 11), (N, N), jnp.float32)
    return jnp.triu(values).reshape(BR, N // BR, BC, N // BC)


def draw_upper_t(key, part):
    values = 0.5 * jax.random.normal(jax.random.fold_in(key, 23), (N, N), jnp.float32)
    lifted = jax.random.uniform(jax.random.fold_in(key, 29), (N,), jnp.float32, 1.0, 2.0)
    return (jnp.triu(values) + jnp.diag(lifted)).reshape(BR, N // BR, BC, N // BC)


def draw_window_starts(key, part):
    round_keys = jax.random.split(jax.random.fold_in(key, 37), ROUNDS)
    picked = jax.vmap(lambda round_key: jax.random.permutation(round_key, N // W)[:NWIN])(round_keys)
    return picked.astype(jnp.int32)


def draw_window_factors(key, part):
    values = jax.random.normal(jax.random.fold_in(key, 41), (ROUNDS, NWIN, 2, W, W), jnp.float32)
    basis, upper = jnp.linalg.qr(values)
    return basis.astype(jnp.float32)


def place_ends(result, own_key, low, top_value):
    longest = result.shape.index(max(result.shape))
    spots = []
    for shift in (0, 1):
        where = [jax.random.randint(jax.random.fold_in(own_key, axis), (), 0, length) for axis, length in enumerate(result.shape)]
        where[longest] = (where[longest] + shift) % result.shape[longest]
        spots.append(tuple(where))
    return result.at[spots[0]].set(low).at[spots[1]].set(top_value)


def level_of(stream_key, dims, pieces, low, largest):
    def one(dim, shards_of):
        draws = jax.random.uniform(jax.random.fold_in(jax.random.fold_in(stream_key, 6), dim), (shards_of,), jnp.float32, low / len(pieces), largest / len(pieces))
        return jnp.repeat(jnp.exp(draws), dims[dim] // shards_of).reshape((-1,) + (1,) * (len(dims) - dim - 1))

    level = one(*pieces[0])
    for cut in pieces[1:]:
        level = level * one(*cut)
    return level


def bell_draw(key, extent, spread, most, shards=(), held_as=jnp.bfloat16):
    result = jax.random.normal(key, extent, jnp.float32) * spread
    if len(shards) > 0:
        result = level_of(key, extent, shards, -0.22, 0.18) * result
    return jnp.clip(result, min=-most, max=most).astype(held_as)


def setup_inputs(seed: int = 0) -> dict:
    key_of = jax.random.split(jax.random.key(seed), 8)
    upper_s = draw_upper_s(jax.random.fold_in(key_of[7], 71), 0)
    upper_t = draw_upper_t(jax.random.fold_in(key_of[7], 71), 0)
    left_vectors = bell_draw(key_of[2], (BR, N_ROW * W, BC, N_COL * W), 1.0, 6.0, ((1, 16), (3, 8)), jnp.float32)
    right_vectors = bell_draw(key_of[3], (BR, N_ROW * W, BC, N_COL * W), 1.0, 6.0, ((1, 16), (3, 8)), jnp.float32)
    window_starts = draw_window_starts(jax.random.fold_in(key_of[7], 71), 0)
    selection = place_ends((jax.random.randint(key_of[5], (ROUNDS, NWIN, W), 0, 2) < 1).astype(jnp.int32), jax.random.fold_in(key_of[5], 1), 0, 1)
    window_factors = draw_window_factors(jax.random.fold_in(key_of[7], 71), 0)
    return dict(upper_s=upper_s, upper_t=upper_t, left_vectors=left_vectors, right_vectors=right_vectors, window_starts=window_starts, selection=selection, window_factors=window_factors)


def destinations(flags):
    flags = flags.astype(jnp.int32)
    earlier = (jnp.cumsum(flags) - flags).astype(jnp.int32)
    chosen = jnp.sum(flags).astype(jnp.int32)
    position = jnp.arange(flags.shape[0], dtype=jnp.int32)
    return jnp.where(flags == 1, earlier, chosen + position - earlier).astype(jnp.int32)

def window_bases(factors, flags):
    target = destinations(flags)
    return (jnp.take(factors[0], target, axis=0), jnp.take(factors[1], target, axis=0))

def product(left, right):
    return jnp.dot(left.astype(jnp.float32), right.astype(jnp.float32), precision=lax.Precision.HIGHEST, preferred_element_type=jnp.float32)

def reference(upper_s, upper_t, left_vectors, right_vectors, window_starts, selection, window_factors):
    mats = (upper_s.reshape(N, N), upper_t.reshape(N, N), left_vectors.reshape(N, N), right_vectors.reshape(N, N))
    for round_idx in range(ROUNDS):

        def apply_window(index, state):
            pencil_s, pencil_t, left_basis, right_basis = state
            left_factor, right_factor = window_bases(window_factors[round_idx, index], selection[round_idx, index])
            offset = (window_starts[round_idx, index] * W).astype(jnp.int32)
            band_s = lax.dynamic_slice_in_dim(pencil_s, offset, W, 0)
            pencil_s = lax.dynamic_update_slice_in_dim(pencil_s, product(left_factor.T, band_s), offset, 0)
            band_t = lax.dynamic_slice_in_dim(pencil_t, offset, W, 0)
            pencil_t = lax.dynamic_update_slice_in_dim(pencil_t, product(left_factor.T, band_t), offset, 0)
            strip_s = lax.dynamic_slice_in_dim(pencil_s, offset, W, 1)
            pencil_s = lax.dynamic_update_slice_in_dim(pencil_s, product(strip_s, right_factor), offset, 1)
            strip_t = lax.dynamic_slice_in_dim(pencil_t, offset, W, 1)
            pencil_t = lax.dynamic_update_slice_in_dim(pencil_t, product(strip_t, right_factor), offset, 1)
            strip_left = lax.dynamic_slice_in_dim(left_basis, offset, W, 1)
            left_basis = lax.dynamic_update_slice_in_dim(left_basis, product(strip_left, left_factor), offset, 1)
            strip_right = lax.dynamic_slice_in_dim(right_basis, offset, W, 1)
            right_basis = lax.dynamic_update_slice_in_dim(right_basis, product(strip_right, right_factor), offset, 1)
            return (pencil_s, pencil_t, left_basis, right_basis)
        mats = lax.fori_loop(0, NWIN, apply_window, mats)
    return tuple((matrix.reshape(BR, N // BR, BC, N // BC) for matrix in mats))
```

```python
import functools

import jax
import jax.numpy as jnp
from jax import lax
from jax.experimental import pallas as pl
from jax.experimental.pallas import tpu as pltpu
from jax.sharding import PartitionSpec as P

F32, BF = jnp.float32, jnp.bfloat16
MESH = pl.DeviceIdType.MESH
ANY = pl.BlockSpec(memory_space=pl.ANY)
VM = pl.BlockSpec(memory_space=pltpu.VMEM)
SM = pl.BlockSpec(memory_space=pltpu.SMEM)
W = 256
NQ, NC, NB, NK = 8, 8, 4, 3


def split(x):
    hi = x.astype(BF)
    return hi, (x - hi.astype(F32)).astype(BF)


def mm(a, b):
    d = functools.partial(jnp.dot, preferred_element_type=F32)
    return d(a[0], b[0]) + (d(a[0], b[1]) + d(a[1], b[0]))


def permute_kernel(starts, sel, wf, send, inv):
    r, c = lax.axis_index("row"), lax.axis_index("col")
    lane = lax.broadcasted_iota(jnp.int32, (32, W), 1)
    pos = lax.broadcasted_iota(jnp.int32, (32, W), 0) + c * 32
    pos1 = lax.broadcasted_iota(jnp.int32, (32, 1), 0) + c * 32
    win = lax.broadcasted_iota(jnp.int32, (16, 16), 0)
    win_l = lax.broadcasted_iota(jnp.int32, (16, 16), 1)
    blk = lax.broadcasted_iota(jnp.int32, (16, 32), 1)
    win_b = lax.broadcasted_iota(jnp.int32, (16, 32), 0)
    for k in range(NK):
        flags = jnp.broadcast_to(sel[k, pl.ds(r, 1), :], (32, W))
        earlier = jnp.sum(jnp.where(lane < pos, flags, 0), axis=1, keepdims=True)
        own = jnp.sum(jnp.where(lane == pos, flags, 0), axis=1, keepdims=True)
        chosen = jnp.sum(flags, axis=1, keepdims=True)
        target = jnp.where(own == 1, earlier, chosen + pos1 - earlier)
        onehot = jnp.where(lane == target, 1.0, 0.0).astype(BF)
        for x in range(2):
            f = wf[k, 0, x]
            hi = f.astype(BF)
            rest = f - hi.astype(F32)
            mid = rest.astype(BF)
            lo = (rest - mid.astype(F32)).astype(BF)
            d = functools.partial(jnp.dot, preferred_element_type=F32)
            rows = (d(onehot, hi) + d(onehot, mid)) + d(onehot, lo)
            for q in range(NQ):
                send[q, x, k] = rows[(q // 2) * 8:(q // 2) * 8 + 8, (q % 2) * 128:(q % 2) * 128 + 128]
        st = jnp.broadcast_to(starts[k:k + 1, :], (16, 16))
        col = jnp.sum(jnp.where(win == win_l, st, 0), axis=1, keepdims=True)
        inv[k:k + 1, :] = 16 + jnp.sum(jnp.where(col == blk, win_b - 16, 0), axis=0, keepdims=True)


def task_chip(b, x, c):
    xx = (c // 4 + x + 2 * (b % 2)) % 4
    flip = b // 2
    y = (flip + (1 - x) * ((c // 2) % 2)) % 2
    return xx * 2 + y


def comm_kernel(inv, send_a, colf, rowl, recv_a, send_b, recv_b, combo,
                a_send, a_recv, b_send, b_recv, c_send, c_recv, d_send, d_recv, e_send, e_recv):
    r, c = lax.axis_index("row"), lax.axis_index("col")
    q, s = r // 2, r % 2
    rt, lt = c * 4 + q // 2, q % 2
    bx = (q // 2 + 4 - c // 4) % 4
    task_x = bx % 2
    is_task = task_x == s
    task_b = bx // 2 + 2 * jnp.where(task_x == 0, (q + c // 2) % 2, q % 2)

    def put(src, dst, ssem, rsem, rr, cc):
        me = jnp.logical_and(rr == r, cc == c)

        @pl.when(me)
        def _():
            pltpu.make_async_copy(src, dst, rsem).start()

        @pl.when(jnp.logical_not(me))
        def _():
            pltpu.make_async_remote_copy(src, dst, ssem, rsem, device_id=(rr, cc), device_id_type=MESH).start()

    def wait_for(ref, sem):
        pltpu.make_async_copy(ref, ref, sem).wait()

    def spread(i, _):
        rr = (r + i) % 16
        put(send_a.at[rr // 2, rr % 2], recv_a.at[r], a_send, a_recv, rr, c)
        return 0

    lax.fori_loop(0, 16, spread, 0)
    ident = jnp.where(
        lax.broadcasted_iota(jnp.int32, (8, 128), 0) + rt * 8
        == lax.broadcasted_iota(jnp.int32, (8, 128), 1) + lt * 128, 1.0, 0.0).astype(F32)
    for k in range(NK):
        recv_a[16, k] = ident
    wait_for(recv_a.at[pl.ds(0, 16)], a_recv)

    def pick(i, _):
        for k in range(NK):
            send_b[i, k] = recv_a[inv[k, i], k]
        return 0

    lax.fori_loop(0, 32, pick, 0)

    def gather(i, _):
        cc, b = (c + i // NB) % NC, i % NB
        put(send_b.at[cc + 8 * b],
            recv_b.at[:, pl.ds(pl.multiple_of(rt * 8, 8), 8), pl.ds(pl.multiple_of(lt * 128, 128), 128)],
            b_send, b_recv, task_chip(b, s, cc) * 2 + s, cc)
        return 0

    lax.fori_loop(0, 32, gather, 0)

    @pl.when(is_task)
    def _():
        wait_for(recv_b, b_recv)
        combo[...] = mm(split(mm(split(recv_b[0]), split(recv_b[1]))), split(recv_b[2]))
        slot = task_x * NB + task_b

        def tell(i, _):
            rr = (r + i) % 16
            half = pl.ds(pl.multiple_of((rr % 2) * 128, 128), 128)
            put(combo.at[half], colf.at[slot, half], c_send, c_recv.at[slot], rr, c)
            return 0

        lax.fori_loop(0, 16, tell, 0)

        @pl.when(task_x == 0)
        def _():
            def tell_row(i, _):
                put(combo, rowl.at[task_b // 2], d_send, d_recv, c + 8 * (task_b % 2), (c + i) % NC)
                return 0

            lax.fori_loop(0, NC, tell_row, 0)

    half = pl.ds(pl.multiple_of(s * 128, 128), 128)
    other = pl.ds(pl.multiple_of((1 - s) * 128, 128), 128)

    def forward(i, _):
        wait_for(colf.at[i, half], c_recv.at[i])
        pltpu.make_async_remote_copy(colf.at[i, half], colf.at[i, half], e_send, e_recv,
                                     device_id=(r + 1 - 2 * s, c), device_id_type=MESH).start()
        return 0

    lax.fori_loop(0, 8, forward, 0)
    wait_for(rowl, d_recv)
    wait_for(colf.at[:, other], e_recv)
    wait_for(colf.at[:, half], e_send)
    wait_for(recv_a.at[pl.ds(0, 15)], a_send)

    @pl.when(is_task)
    def _():
        wait_for(send_b.at[pl.ds(0, 31)], b_send)
        wait_for(colf.at[:, pl.ds(0, 240)], c_send)

        @pl.when(task_x == 0)
        def _():
            mine = c + 8 * (task_b % 2) == r

            @pl.when(mine)
            def _():
                wait_for(colf.at[pl.ds(0, 7)], d_send)

            @pl.when(jnp.logical_not(mine))
            def _():
                wait_for(colf, d_send)

    @pl.when(jnp.logical_not(is_task))
    def _():
        wait_for(send_b, b_send)


def comm_call(inv, send_a):
    dma = pltpu.SemaphoreType.DMA
    return pl.pallas_call(
        comm_kernel,
        out_shape=[jax.ShapeDtypeStruct((2 * NB, W, W), F32), jax.ShapeDtypeStruct((2, W, W), F32)],
        in_specs=[SM, VM],
        out_specs=[ANY, ANY],
        scratch_shapes=[
            pltpu.VMEM((17, NK, 8, 128), F32), pltpu.VMEM((32, NK, 8, 128), F32),
            pltpu.VMEM((NK, W, W), F32), pltpu.VMEM((W, W), F32),
            dma, dma, dma, dma, dma, dma((8,)), dma, dma, dma, dma,
        ],
        compiler_params=pltpu.CompilerParams(has_side_effects=True, vmem_limit_bytes=12 * 1024 * 1024),
        name="comm",
    )(inv, send_a)


def permute_call(starts, sel, wf):
    return pl.pallas_call(
        permute_kernel,
        out_shape=[jax.ShapeDtypeStruct((NQ, 2, NK, 8, 128), F32), jax.ShapeDtypeStruct((NK, 32), jnp.int32)],
        in_specs=[VM, VM, VM],
        out_specs=[VM, VM],
        name="permute",
    )(starts, sel, wf)


def apply_kernel(s, t, q, z, colf, rowl, os, ot, oq, oz, buf, obuf, ch, cl, rh, rl, in_sem, out_sem):
    br, w, bc, _ = s.shape
    mats, outs = (s, t, q, z), (os, ot, oq, oz)
    def load(m, a, b):
        return pltpu.make_async_copy(mats[m].at[a, :, b, :], buf.at[m, a * bc + b], in_sem.at[m, a * bc + b])
    def store(m, a, b):
        return pltpu.make_async_copy(obuf.at[m, a * bc + b], outs[m].at[a, :, b, :], out_sem.at[m, a * bc + b])
    for a in range(br):
        for b in range(bc):
            for m in range(4):
                load(m, a, b).start()
    for a in range(br):
        h, l = split(rowl[a].T)
        rh[a], rl[a] = h, l
    def cs(i, _):
        h, l = split(colf[i])
        ch[i], cl[i] = h, l
        return 0
    lax.fori_loop(0, 2 * bc, cs, 0)
    def step(i, _):
        a, b = i // bc, i % bc
        for m in range(4):
            load(m, a, b).wait()
        left = (ch[b], cl[b])
        right = (ch[bc + b], cl[bc + b])
        row = (rh[a], rl[a])
        for m in range(4):
            x = split(buf[m, i])
            y = mm(x, left if m == 2 else right)
            if m < 2:
                y = mm(row, split(y))
            obuf[m, i] = y
            store(m, a, b).start()
        return 0
    lax.fori_loop(0, br * bc, step, 0)
    for a in range(br):
        for b in range(bc):
            for m in range(4):
                store(m, a, b).wait()

def apply_call(s, t, q, z, colf, rowl):
    br, w, bc, _ = s.shape
    return pl.pallas_call(
        apply_kernel,
        out_shape=[jax.ShapeDtypeStruct(s.shape, F32)] * 4,
        in_specs=[ANY] * 4 + [VM, VM],
        out_specs=[ANY] * 4,
        scratch_shapes=[
            pltpu.VMEM((4, br * bc, w, w), F32), pltpu.VMEM((4, br * bc, w, w), F32),
            pltpu.VMEM((2 * bc, w, w), BF), pltpu.VMEM((2 * bc, w, w), BF),
            pltpu.VMEM((br, w, w), BF), pltpu.VMEM((br, w, w), BF),
            pltpu.SemaphoreType.DMA((4, br * bc)), pltpu.SemaphoreType.DMA((4, br * bc)),
        ],
        compiler_params=pltpu.CompilerParams(vmem_limit_bytes=40 * 1024 * 1024),
        name="apply",
    )(s, t, q, z, colf, rowl)


def shards(s, t, q, z, starts, sel, wf):
    send, inv = permute_call(starts, sel, wf)
    colf, rowl = comm_call(inv, send)
    return apply_call(s, t, q, z, colf, rowl)


def solution(mesh):
    spec = P(None, "row", None, "col")
    return jax.shard_map(
        shards,
        mesh=mesh,
        in_specs=(spec,) * 4 + (P(), P(), P(None, "row")),
        out_specs=(spec,) * 4,
        check_vma=False,
    )
```

```python
import functools

import jax
import jax.numpy as jnp
from jax import lax
from jax.experimental import pallas as pl
from jax.experimental.pallas import tpu as pltpu
from jax.sharding import PartitionSpec as P

F32, BF = jnp.float32, jnp.bfloat16
MESH = pl.DeviceIdType.MESH
ANY = pl.BlockSpec(memory_space=pl.ANY)
VM = pl.BlockSpec(memory_space=pltpu.VMEM)
W = 256
NQ, NC, NB, NK = 8, 8, 4, 3


def div(a, b):
    return lax.div(a, jnp.int32(b))


def rem(a, b):
    return lax.rem(a, jnp.int32(b))


def split(x):
    hi = x.astype(BF)
    return hi, (x - hi.astype(F32)).astype(BF)


def mm(a, b):
    d = functools.partial(jnp.dot, preferred_element_type=F32)
    return d(a[0], b[0]) + (d(a[0], b[1]) + d(a[1], b[0]))

NT = 2 * NB


def permute_rows(sel, wf, send, r, c):
    lane = lax.broadcasted_iota(jnp.int32, (32, W), 1)
    pos = lax.broadcasted_iota(jnp.int32, (32, W), 0) + c * 32
    pos1 = lax.broadcasted_iota(jnp.int32, (32, 1), 0) + c * 32
    for k in range(NK):
        flags = jnp.broadcast_to(sel[k, pl.ds(r, 1), :], (32, W))
        earlier = jnp.sum(jnp.where(lane < pos, flags, 0), axis=1, keepdims=True)
        own = jnp.sum(jnp.where(lane == pos, flags, 0), axis=1, keepdims=True)
        chosen = jnp.sum(flags, axis=1, keepdims=True)
        target = jnp.where(own == 1, earlier, chosen + pos1 - earlier)
        onehot = jnp.where(lane == target, 1.0, 0.0).astype(BF)
        for x in range(2):
            f = wf[k, x]
            hi = f.astype(BF)
            rest = f - hi.astype(F32)
            mid = rest.astype(BF)
            lo = (rest - mid.astype(F32)).astype(BF)
            d = functools.partial(jnp.dot, preferred_element_type=F32)
            rows = (d(onehot, hi) + d(onehot, mid)) + d(onehot, lo)
            for q in range(NQ):
                send[q, x, k] = rows[(q // 2) * 8:(q // 2) * 8 + 8, (q % 2) * 128:(q % 2) * 128 + 128]


def window_of_block(starts, inv):
    win = lax.broadcasted_iota(jnp.int32, (16, 16), 0)
    win_l = lax.broadcasted_iota(jnp.int32, (16, 16), 1)
    blk = lax.broadcasted_iota(jnp.int32, (16, 128), 1)
    win_b = lax.broadcasted_iota(jnp.int32, (16, 128), 0)
    for k in range(NK):
        st = jnp.broadcast_to(starts[k:k + 1, :], (16, 16))
        col = jnp.sum(jnp.where(win == win_l, st, 0), axis=1, keepdims=True)
        inv[k:k + 1, :] = 16 - jnp.max(jnp.where(col == blk, 16 - win_b, 0), axis=0, keepdims=True)


def task_chip(b, x, c):
    b, c = jnp.int32(b), jnp.int32(c)
    xx = rem(div(c, 4) + x + 2 * rem(b, 2), 4)
    y = rem(div(b, 2) + (1 - x) * rem(div(c, 2), 2), 2)
    return xx * 2 + y


def task_of(xx, y, c):
    bx = rem(xx + 4 - div(c, 4), 4)
    kind = rem(bx, 2)
    return kind, div(bx, 2) + 2 * rem(y + (1 - kind) * rem(div(c, 2), 2), 2)


def comm_kernel(starts_in, sel_in, wf, s_in, t_in, q_in, z_in, rowl, xs, colf, ch, cl,
                starts, sel, wf_v, send_a, inv_v, inv, recv_a, send_b, recv_b, combo, raw,
                ready, s_sem, w_sem, i_sem, raw_sem, x_sem, a_send, a_recv, b_send, b_recv,
                o_send, c_send, c_recv, e_send, e_recv, t_send, d_send, d_recv):
    r, c = lax.axis_index("row"), lax.axis_index("col")
    x, y, h = div(r, 4), rem(div(r, 2), 2), rem(r, 2)
    q, z = div(r, 2), div(c, 2)
    rt, lt = c * 4 + div(q, 2), rem(q, 2)
    kind, task_b = task_of(x, y, c)
    is_task = kind == h

    barrier = pltpu.get_barrier_semaphore()

    def signal(sem, rr, cc):
        pl.semaphore_signal(sem, inc=1, device_id=(rr, cc), device_id_type=MESH)

    for i in (4, 5, 3, 2, 6, 1, 7):
        signal(barrier, r, rem(c + i, NC))
    for i in range(1, 16):
        signal(barrier, rem(r + i, 16), c)

    def remote(src, dst, ssem, rsem, rr, cc):
        pltpu.make_async_remote_copy(src, dst, ssem, rsem, device_id=(rr, cc), device_id_type=MESH).start()

    def put(src, dst, ssem, rsem, rr, cc):
        me = jnp.logical_and(rr == r, cc == c)

        @pl.when(me)
        def _():
            pltpu.make_async_copy(src, dst, rsem).start()

        @pl.when(jnp.logical_not(me))
        def _():
            remote(src, dst, ssem, rsem, rr, cc)

    def wait_for(ref, sem):
        pltpu.make_async_copy(ref, ref, sem).wait()

    load_i = [pltpu.make_async_copy(starts_in, starts, s_sem.at[0]), pltpu.make_async_copy(sel_in, sel, s_sem.at[1])]
    for copy in load_i:
        copy.start()
    load_w = pltpu.make_async_copy(wf.at[:, 0], wf_v, w_sem)
    load_w.start()
    load_x = [pltpu.make_async_copy(m, raw.at[i], raw_sem.at[i]) for i, m in enumerate((s_in, t_in, q_in, z_in))]
    for copy in load_x:
        copy.start()
    for copy in load_i:
        copy.wait()
    window_of_block(starts, inv_v)
    ident = jnp.where(
        lax.broadcasted_iota(jnp.int32, (8, 128), 0) + rt * 8
        == lax.broadcasted_iota(jnp.int32, (8, 128), 1) + lt * 128, 1.0, 0.0).astype(F32)
    for k in range(NK):
        recv_a[16, k] = ident
    load_w.wait()
    permute_rows(sel, wf_v, send_a, r, c)
    move_inv = pltpu.make_async_copy(inv_v, inv, i_sem)
    move_inv.start()

    pl.semaphore_wait(barrier, 15 + NC - 1)

    for i in range(1, 16):
        rr = rem(r + i, 16)
        remote(send_a.at[div(rr, 2), rem(rr, 2)], recv_a.at[r], a_send, a_recv, rr, c)
    pltpu.make_async_copy(send_a.at[q, h], recv_a.at[r], a_recv).start()
    for i in (4, 5, 3, 2, 6, 1, 7):
        signal(ready, r, rem(c + i, NC))
    for copy in load_x:
        copy.wait()
    for i in range(4):
        for a in range(2):
            for b in range(NB):
                pltpu.make_async_copy(raw.at[i, a, :, b, :], xs.at[i, b, pl.ds(a * W, W)], x_sem).start()
    move_inv.wait()
    pl.semaphore_wait(ready, NC - 1)
    wait_for(recv_a.at[pl.ds(0, 16)], a_recv)

    place = recv_b.at[:, pl.ds(pl.multiple_of(rt * 8, 8), 8), pl.ds(pl.multiple_of(lt * 128, 128), 128)]
    for i in range(32):
        for k in range(NK):
            send_b[i, k] = recv_a[inv[k, i], k]
    for i in (4, 5, 3, 2, 6, 1, 7):
        cc = rem(c + i, NC)
        for b in range(NB):
            remote(send_b.at[cc + NC * b], place, b_send, b_recv, task_chip(b, h, cc) * 2 + h, cc)
    for i in range(1, NB):
        b = rem(task_b + i, NB)
        remote(send_b.at[c + NC * b], place, b_send, b_recv, task_chip(b, h, c) * 2 + h, c)
    put(send_b.at[c + NC * task_b], place, b_send, b_recv, task_chip(task_b, h, c) * 2 + h, c)

    def part(first, count):
        return pl.ds(pl.multiple_of(first, 64), count)

    mine, theirs = part(h * 128, 128), part((1 - h) * 128, 128)
    near, far = part(h * 128, 64), part(h * 128 + 64, 64)
    partner = r + 1 - 2 * h

    def slot_at(dx, dy):
        kk, bb = task_of(rem(x + dx, 4), rem(y + dy, 2), c)
        return kk * NB + bb

    own = kind * NB + task_b

    @pl.when(is_task)
    def _():
        wait_for(recv_b, b_recv)
        combo[...] = mm(split(mm(split(recv_b[0]), split(recv_b[1]))), split(recv_b[2]))
        pltpu.make_async_copy(combo.at[mine], colf.at[own, mine], c_recv.at[0]).start()
        remote(combo.at[theirs], colf.at[own, theirs], o_send, c_recv.at[0], partner, c)
        pltpu.make_async_copy(combo.at[theirs], colf.at[own, theirs], e_recv).start()

        @pl.when(kind == 0)
        def _():
            for p in range(2):
                rows = pl.ds(p * 128, 128)
                put(combo.at[rows], rowl.at[div(task_b, 2), rows], t_send, d_recv.at[div(task_b, 2), p],
                    c + NC * (rem(task_b, 2)), c)
                remote(combo.at[rows], rowl.at[div(task_b, 2), rows], t_send, d_recv.at[div(task_b, 2), p],
                       c + NC * (rem(task_b, 2)), c + 1 - 2 * rem(c, 2))

    left, right = rem(r + 12, 16), rem(r + 4, 16)
    across = x * 4 + (1 - y) * 2 + h

    def got(slot, rows, i):
        wait_for(colf.at[slot, rows], c_recv.at[i])

    def pass_on(slot, rows, i, rr):
        remote(colf.at[slot, rows], colf.at[slot, rows], c_send, c_recv.at[i], rr, c)

    def share(slot):
        remote(colf.at[slot, mine], colf.at[slot, mine], e_send, e_recv, partner, c)

    zd = rem(z + 4 - div(rem(r, NC), 2), 4)

    def got_row(a, p):
        wait_for(rowl.at[a, pl.ds(p * 128, 128)], d_recv.at[a, p])

    def pass_row(a, p):
        rows = pl.ds(p * 128, 128)
        remote(rowl.at[a, rows], rowl.at[a, rows], d_send, d_recv.at[a, p], r, rem(c + (2 if p == 0 else NC - 2), NC))

    got(own, mine, 0)
    pass_on(own, near, 1, right)
    pass_on(own, far, 4, left)
    pass_on(own, near, 5, across)
    pass_on(own, far, 2, right)
    pass_on(own, near, 3, left)
    pass_on(own, far, 6, across)

    @pl.when(is_task)
    def _():
        share(own)

    @pl.when(zd == 0)
    def _():
        for a in range(2):
            for p in range(2):
                got_row(a, p)
                pass_row(a, p)

    at_left, at_right, at_across = slot_at(3, 0), slot_at(1, 0), slot_at(0, 1)
    got(at_left, near, 1)
    pass_on(at_left, near, 7, right)
    pass_on(at_left, near, 9, across)
    got(at_right, far, 4)
    pass_on(at_right, far, 8, left)
    pass_on(at_right, far, 12, across)
    got(at_across, near, 5)
    pass_on(at_across, near, 11, left)
    got(at_across, far, 6)
    pass_on(at_across, far, 10, right)
    share(at_across)

    @pl.when(zd == 1)
    def _():
        for a in range(2):
            got_row(a, 0)
            pass_row(a, 0)

    @pl.when(zd == 3)
    def _():
        for a in range(2):
            got_row(a, 1)
            pass_row(a, 1)

    got(at_left, far, 2)
    share(at_left)
    got(at_right, near, 3)
    share(at_right)
    across_left, across_right = slot_at(3, 1), slot_at(1, 1)
    got(across_left, near, 9)
    pass_on(across_left, near, 13, right)
    got(across_right, far, 12)
    pass_on(across_right, far, 14, left)
    got(across_left, far, 10)
    share(across_left)
    got(across_right, near, 11)
    share(across_right)

    @pl.when(zd == 2)
    def _():
        for a in range(2):
            for p in range(2):
                got_row(a, p)
                pass_row(a, p)

    opposite, across_opposite = slot_at(2, 0), slot_at(2, 1)
    got(opposite, near, 7)
    got(opposite, far, 8)
    share(opposite)
    got(across_opposite, near, 13)
    got(across_opposite, far, 14)
    share(across_opposite)

    wait_for(xs, x_sem)
    wait_for(recv_a.at[pl.ds(0, 15)], a_send)
    wait_for(colf.at[:, theirs], e_recv)

    def halves(i, _):
        ch[i], cl[i] = split(colf[i])
        return 0

    def columns(b, _):
        for m in range(4):
            f = b if m == 2 else NB + b
            xs[m, b] = mm(split(xs[m, b]), (ch[f], cl[f]))
        return 0

    lax.fori_loop(0, NT, halves, 0)
    lax.fori_loop(0, NB, columns, 0)
    wait_for(colf.at[pl.ds(0, 7), mine], c_send)

    @pl.when(zd == 1)
    def _():
        got_row(0, 1)
        got_row(1, 1)

    @pl.when(zd == 3)
    def _():
        got_row(0, 0)
        got_row(1, 0)

    @pl.when(zd % 2 == 0)
    def _():
        wait_for(rowl, d_send)

    @pl.when(zd % 2 == 1)
    def _():
        wait_for(rowl.at[0], d_send)

    @pl.when(is_task)
    def _():
        wait_for(send_b.at[pl.ds(0, 31)], b_send)
        wait_for(combo.at[theirs], o_send)
        wait_for(colf.at[:, mine], e_send)

        @pl.when(kind == 0)
        def _():
            local = c + NC * (rem(task_b, 2)) == r

            @pl.when(local)
            def _():
                wait_for(rowl.at[0], t_send)

            @pl.when(jnp.logical_not(local))
            def _():
                wait_for(rowl, t_send)

    @pl.when(jnp.logical_not(is_task))
    def _():
        wait_for(send_b, b_send)
        wait_for(colf.at[pl.ds(0, 7), mine], e_send)


def comm_call(starts, sel, wf, s, t, q, z):
    dma = pltpu.SemaphoreType.DMA
    br, w, bc, _ = s.shape
    return pl.pallas_call(
        comm_kernel,
        out_shape=[
            pltpu.VMEM((br, W, W), F32), pltpu.VMEM((4, bc, br * w, w), F32),
        ],
        in_specs=[pl.BlockSpec(memory_space=pltpu.HBM)] * 7,
        out_specs=[VM, VM],
        scratch_shapes=[
            pltpu.VMEM((NT, W, W), F32), pltpu.VMEM((NT, W, W), BF), pltpu.VMEM((NT, W, W), BF),
            pltpu.VMEM(starts.shape, jnp.int32), pltpu.VMEM(sel.shape, jnp.int32),
            pltpu.VMEM((NK, 2, W, W), F32), pltpu.VMEM((NQ, 2, NK, 8, 128), F32),
            pltpu.VMEM((8, 128), jnp.int32), pltpu.SMEM((8, 128), jnp.int32),
            pltpu.VMEM((17, NK, 8, 128), F32), pltpu.VMEM((32, NK, 8, 128), F32),
            pltpu.VMEM((NK, W, W), F32), pltpu.VMEM((W, W), F32), pltpu.VMEM((4, br, w, bc, w), F32),
            pltpu.SemaphoreType.REGULAR, dma((2,)), dma, dma, dma((4,)), dma, dma, dma, dma, dma,
            dma, dma, dma((15,)), dma, dma, dma, dma, dma((2, 2)),
        ],
        compiler_params=pltpu.CompilerParams(has_side_effects=True, vmem_limit_bytes=24 * 1024 * 1024, collective_id=0),
        name="comm",
    )(*(pltpu.with_memory_space_constraint(v, pltpu.HBM) for v in (starts, sel, wf, s, t, q, z)))


def finish_kernel(xs, rowl, os, ot, oq, oz, obuf, rh, rl, out_sem):
    _, bc, rows, w = xs.shape
    br = rows // w
    outs = (os, ot, oq, oz)

    def store(src, m, a, b):
        pltpu.make_async_copy(src.at[m, b, pl.ds(a * w, w)], outs[m].at[a, :, b, :], out_sem).start()

    for b in range(bc):
        for m in range(2, 4):
            for a in range(br):
                store(xs, m, a, b)
    for a in range(br):
        rh[a], rl[a] = split(rowl[a].T)

    def row_blocks(b, _):
        for m in range(2):
            for a in range(br):
                part = pl.ds(a * w, w)
                obuf[m, b, part] = mm((rh[a], rl[a]), split(xs[m, b, part]))
        for m in range(2):
            for a in range(br):
                store(obuf, m, a, b)
        return 0

    lax.fori_loop(0, bc, row_blocks, 0)
    pltpu.make_async_copy(xs, xs, out_sem).wait()


def finish_call(shape, xs, rowl):
    br, w, bc, _ = shape
    return pl.pallas_call(
        finish_kernel,
        out_shape=[jax.ShapeDtypeStruct(shape, F32)] * 4,
        in_specs=[VM, VM],
        out_specs=[ANY] * 4,
        scratch_shapes=[
            pltpu.VMEM((2,) + xs.shape[1:], F32),
            pltpu.VMEM((br, w, w), BF), pltpu.VMEM((br, w, w), BF),
            pltpu.SemaphoreType.DMA,
        ],
        compiler_params=pltpu.CompilerParams(vmem_limit_bytes=24 * 1024 * 1024),
        name="finish",
    )(xs, rowl)


def shards(s, t, q, z, starts, sel, wf):
    rowl, xs = comm_call(starts, sel, wf, s, t, q, z)
    return finish_call(s.shape, xs, rowl)


def solution(mesh):
    spec = P(None, "row", None, "col")
    return jax.shard_map(
        shards,
        mesh=mesh,
        in_specs=(spec,) * 4 + (P(), P(), P(None, "row")),
        out_specs=(spec,) * 4,
        check_vma=False,
    )
```

```python
import functools

import jax
import jax.numpy as jnp
from jax import lax
from jax.experimental import pallas as pl
from jax.experimental.pallas import tpu as pltpu
from jax.sharding import PartitionSpec as P

F32, BF = jnp.float32, jnp.bfloat16
MESH = pl.DeviceIdType.MESH
ANY = pl.BlockSpec(memory_space=pl.ANY)
VM = pl.BlockSpec(memory_space=pltpu.VMEM)
W = 256
NQ, NC, NB, NK = 8, 8, 4, 3


def div(a, b):
    return lax.div(a, jnp.int32(b))


def rem(a, b):
    return lax.rem(a, jnp.int32(b))


def split(x):
    hi = x.astype(BF)
    return hi, (x - hi.astype(F32)).astype(BF)


def mm(a, b):
    d = functools.partial(jnp.dot, preferred_element_type=F32)
    return d(a[0], b[0]) + (d(a[0], b[1]) + d(a[1], b[0]))

NT = 2 * NB
SUB, DSUB = 2, 4


def permute_rows(sel, wf, send, r, c):
    lane = lax.broadcasted_iota(jnp.int32, (32, W), 1)
    pos = lax.broadcasted_iota(jnp.int32, (32, W), 0) + c * 32
    pos1 = lax.broadcasted_iota(jnp.int32, (32, 1), 0) + c * 32
    for k in range(NK):
        flags = jnp.broadcast_to(sel[k, pl.ds(r, 1), :], (32, W))
        earlier = jnp.sum(jnp.where(lane < pos, flags, 0), axis=1, keepdims=True)
        own = jnp.sum(jnp.where(lane == pos, flags, 0), axis=1, keepdims=True)
        chosen = jnp.sum(flags, axis=1, keepdims=True)
        target = jnp.where(own == 1, earlier, chosen + pos1 - earlier)
        onehot = jnp.where(lane == target, 1.0, 0.0).astype(BF)
        for x in range(2):
            f = wf[k, x]
            hi = f.astype(BF)
            rest = f - hi.astype(F32)
            mid = rest.astype(BF)
            lo = (rest - mid.astype(F32)).astype(BF)
            d = functools.partial(jnp.dot, preferred_element_type=F32)
            rows = (d(onehot, hi) + d(onehot, mid)) + d(onehot, lo)
            for q in range(NQ):
                send[q, x, k] = rows[(q // 2) * 8:(q // 2) * 8 + 8, (q % 2) * 128:(q % 2) * 128 + 128]


def window_of_block(starts, inv):
    win = lax.broadcasted_iota(jnp.int32, (16, 16), 0)
    win_l = lax.broadcasted_iota(jnp.int32, (16, 16), 1)
    blk = lax.broadcasted_iota(jnp.int32, (16, 128), 1)
    win_b = lax.broadcasted_iota(jnp.int32, (16, 128), 0)
    for k in range(NK):
        st = jnp.broadcast_to(starts[k:k + 1, :], (16, 16))
        col = jnp.sum(jnp.where(win == win_l, st, 0), axis=1, keepdims=True)
        inv[k:k + 1, :] = 16 - jnp.max(jnp.where(col == blk, 16 - win_b, 0), axis=0, keepdims=True)


def task_chip(b, x, c):
    b, c = jnp.int32(b), jnp.int32(c)
    xx = rem(div(c, 4) + x + 2 * rem(b, 2), 4)
    y = rem(div(b, 2) + (1 - x) * rem(div(c, 2), 2), 2)
    return xx * 2 + y


def task_of(xx, y, c):
    bx = rem(xx + 4 - div(c, 4), 4)
    kind = rem(bx, 2)
    return kind, div(bx, 2) + 2 * rem(y + (1 - kind) * rem(div(c, 2), 2), 2)


def comm_kernel(starts_in, sel_in, wf, s_in, t_in, q_in, z_in, rowl, xs, colf, ch, cl,
                starts, sel, wf_v, send_a, inv_v, inv, recv_a, send_b, recv_b, combo, raw,
                ready, s_sem, w_sem, i_sem, raw_sem, x_sem, a_send, a_recv, b_send, b_recv,
                o_send, o_recv, c_send, c_recv, e_send, e_recv, t_send, d_send, d_recv):
    r, c = lax.axis_index("row"), lax.axis_index("col")
    x, y, h = div(r, 4), rem(div(r, 2), 2), rem(r, 2)
    q, z = div(r, 2), div(c, 2)
    rt, lt = c * 4 + div(q, 2), rem(q, 2)
    kind, task_b = task_of(x, y, c)
    is_task = kind == h

    barrier = pltpu.get_barrier_semaphore()

    def signal(sem, rr, cc):
        pl.semaphore_signal(sem, inc=1, device_id=(rr, cc), device_id_type=MESH)

    load_i = [pltpu.make_async_copy(starts_in, starts, s_sem.at[0]), pltpu.make_async_copy(sel_in, sel, s_sem.at[1])]
    for copy in load_i:
        copy.start()
    load_w = pltpu.make_async_copy(wf.at[:, 0], wf_v, w_sem)
    load_w.start()
    for i in (4, 5, 3, 2, 6, 1, 7):
        signal(barrier, r, rem(c + i, NC))
    for i in range(1, 16):
        signal(barrier, rem(r + i, 16), c)

    def remote(src, dst, ssem, rsem, rr, cc):
        pltpu.make_async_remote_copy(src, dst, ssem, rsem, device_id=(rr, cc), device_id_type=MESH).start()

    def put(src, dst, ssem, rsem, rr, cc):
        me = jnp.logical_and(rr == r, cc == c)

        @pl.when(me)
        def _():
            pltpu.make_async_copy(src, dst, rsem).start()

        @pl.when(jnp.logical_not(me))
        def _():
            remote(src, dst, ssem, rsem, rr, cc)

    def wait_for(ref, sem):
        pltpu.make_async_copy(ref, ref, sem).wait()

    load_x = [pltpu.make_async_copy(m, raw.at[i], raw_sem.at[i]) for i, m in enumerate((s_in, t_in, q_in, z_in))]
    for copy in load_x:
        copy.start()
    for copy in load_i:
        copy.wait()
    window_of_block(starts, inv_v)
    ident = jnp.where(
        lax.broadcasted_iota(jnp.int32, (8, 128), 0) + rt * 8
        == lax.broadcasted_iota(jnp.int32, (8, 128), 1) + lt * 128, 1.0, 0.0).astype(F32)
    for k in range(NK):
        recv_a[16, k] = ident
    load_w.wait()
    permute_rows(sel, wf_v, send_a, r, c)
    move_inv = pltpu.make_async_copy(inv_v, inv, i_sem)
    move_inv.start()

    pl.semaphore_wait(barrier, 15 + NC - 1)

    for i in range(1, 16):
        rr = rem(r + i, 16)
        remote(send_a.at[div(rr, 2), rem(rr, 2)], recv_a.at[r], a_send, a_recv, rr, c)
    pltpu.make_async_copy(send_a.at[q, h], recv_a.at[r], a_recv).start()
    for i in (4, 5, 3, 2, 6, 1, 7):
        signal(ready, r, rem(c + i, NC))
    move_inv.wait()
    pl.semaphore_wait(ready, NC - 1)
    wait_for(recv_a.at[pl.ds(0, 16)], a_recv)

    place = recv_b.at[:, pl.ds(pl.multiple_of(rt * 8, 8), 8), pl.ds(pl.multiple_of(lt * 128, 128), 128)]
    for i in range(32):
        for k in range(NK):
            send_b[i, k] = recv_a[inv[k, i], k]
    for i in (4, 5, 3, 2, 6, 1, 7):
        cc = rem(c + i, NC)
        for b in range(NB):
            remote(send_b.at[cc + NC * b], place, b_send, b_recv, task_chip(b, h, cc) * 2 + h, cc)
    for i in range(1, NB):
        b = rem(task_b + i, NB)
        remote(send_b.at[c + NC * b], place, b_send, b_recv, task_chip(b, h, c) * 2 + h, c)
    put(send_b.at[c + NC * task_b], place, b_send, b_recv, task_chip(task_b, h, c) * 2 + h, c)

    for copy in load_x:
        copy.wait()
    for i in range(4):
        for a in range(2):
            for b in range(NB):
                pltpu.make_async_copy(raw.at[i, a, :, b, :], xs.at[i, b, pl.ds(a * W, W)], x_sem).start()

    def part(first, count):
        return pl.ds(pl.multiple_of(first, 8), count)

    mine, theirs = part(h * 128, 128), part((1 - h) * 128, 128)
    near, far = 0, 1

    def piece(side, u):
        return part(h * 128 + side * 64 + u * (64 // SUB), 64 // SUB)

    partner = r + 1 - 2 * h

    def slot_at(dx, dy):
        kk, bb = task_of(rem(x + dx, 4), rem(y + dy, 2), c)
        return kk * NB + bb

    def row_piece(p, u):
        return pl.ds(p * 128 + u * (128 // DSUB), 128 // DSUB)

    own = kind * NB + task_b

    @pl.when(is_task)
    def _():
        wait_for(recv_b, b_recv)
        combo[...] = mm(split(mm(split(recv_b[0]), split(recv_b[1]))), split(recv_b[2]))
        pltpu.make_async_copy(combo.at[mine], colf.at[own, mine], o_recv).start()
        remote(combo.at[theirs], colf.at[own, theirs], o_send, o_recv, partner, c)
        pltpu.make_async_copy(combo.at[theirs], colf.at[own, theirs], e_recv).start()

        @pl.when(kind == 0)
        def _():
            for u in range(DSUB):
                for p in range(2):
                    rows = row_piece(p, u)
                    land, arrived = rowl.at[div(task_b, 2), rows], d_recv.at[div(task_b, 2), p, u]
                    put(combo.at[rows], land, t_send, arrived, c + NC * rem(task_b, 2), c)
                    remote(combo.at[rows], land, t_send, arrived, c + NC * rem(task_b, 2), c + 1 - 2 * rem(c, 2))

    left, right = rem(r + 12, 16), rem(r + 4, 16)
    across = x * 4 + (1 - y) * 2 + h

    def got(slot, side, i):
        for u in range(SUB):
            wait_for(colf.at[slot, piece(side, u)], c_recv.at[i, u])

    def send_piece(slot, side, u, i, rr):
        rows = piece(side, u)
        remote(colf.at[slot, rows], colf.at[slot, rows], c_send, c_recv.at[i, u], rr, c)

    def relay(slot, side, i, *hops):
        for u in range(SUB):
            wait_for(colf.at[slot, piece(side, u)], c_recv.at[i, u])
            for j, rr in hops:
                send_piece(slot, side, u, j, rr)

    def share(slot):
        remote(colf.at[slot, mine], colf.at[slot, mine], e_send, e_recv, partner, c)

    zd = rem(z + 4 - div(rem(r, NC), 2), 4)

    def got_row(a, p):
        for u in range(DSUB):
            wait_for(rowl.at[a, row_piece(p, u)], d_recv.at[a, p, u])

    def relay_rows(*sides):
        for u in range(DSUB):
            for a in range(2):
                for p in sides:
                    rows = row_piece(p, u)
                    wait_for(rowl.at[a, rows], d_recv.at[a, p, u])
                    remote(rowl.at[a, rows], rowl.at[a, rows], d_send, d_recv.at[a, p, u],
                           r, rem(c + (2 if p == 0 else NC - 2), NC))

    wait_for(colf.at[own, mine], o_recv)
    for u in range(SUB):
        send_piece(own, near, u, 1, right)
        send_piece(own, far, u, 4, left)
        send_piece(own, near, u, 5, across)
    for u in range(SUB):
        send_piece(own, far, u, 6, across)
        send_piece(own, far, u, 2, right)
        send_piece(own, near, u, 3, left)

    @pl.when(is_task)
    def _():
        share(own)

    @pl.when(zd == 0)
    def _():
        relay_rows(0, 1)

    at_left, at_right, at_across = slot_at(3, 0), slot_at(1, 0), slot_at(0, 1)
    relay(at_left, near, 1, (7, right), (9, across))
    relay(at_right, far, 4, (8, left), (12, across))
    relay(at_across, near, 5, (11, left))
    relay(at_across, far, 6, (10, right))
    share(at_across)

    @pl.when(zd == 1)
    def _():
        relay_rows(0)

    @pl.when(zd == 3)
    def _():
        relay_rows(1)

    got(at_left, far, 2)
    share(at_left)
    got(at_right, near, 3)
    share(at_right)
    across_left, across_right = slot_at(3, 1), slot_at(1, 1)
    relay(across_left, near, 9, (13, right))
    relay(across_right, far, 12, (14, left))

    @pl.when(zd == 2)
    def _():
        relay_rows(0, 1)

    got(across_left, far, 10)
    share(across_left)
    got(across_right, near, 11)
    share(across_right)
    opposite, across_opposite = slot_at(2, 0), slot_at(2, 1)
    got(opposite, near, 7)
    got(opposite, far, 8)
    share(opposite)
    got(across_opposite, near, 13)
    got(across_opposite, far, 14)
    share(across_opposite)

    wait_for(xs, x_sem)
    wait_for(recv_a.at[pl.ds(0, 15)], a_send)
    wait_for(colf.at[:, theirs], e_recv)

    def halves(i, _):
        ch[i], cl[i] = split(colf[i])
        return 0

    def columns(b, _):
        for m in range(4):
            f = b if m == 2 else NB + b
            xs[m, b] = mm(split(xs[m, b]), (ch[f], cl[f]))
        return 0

    lax.fori_loop(0, NT, halves, 0)
    lax.fori_loop(0, NB, columns, 0)
    wait_for(colf.at[pl.ds(0, 7), mine], c_send)

    @pl.when(zd == 1)
    def _():
        got_row(0, 1)
        got_row(1, 1)

    @pl.when(zd == 3)
    def _():
        got_row(0, 0)
        got_row(1, 0)

    @pl.when(zd % 2 == 0)
    def _():
        wait_for(rowl, d_send)

    @pl.when(zd % 2 == 1)
    def _():
        wait_for(rowl.at[0], d_send)

    @pl.when(is_task)
    def _():
        wait_for(send_b.at[pl.ds(0, 31)], b_send)
        wait_for(combo.at[theirs], o_send)
        wait_for(colf.at[:, mine], e_send)

        @pl.when(kind == 0)
        def _():
            local = c + NC * (rem(task_b, 2)) == r

            @pl.when(local)
            def _():
                wait_for(rowl.at[0], t_send)

            @pl.when(jnp.logical_not(local))
            def _():
                wait_for(rowl, t_send)

    @pl.when(jnp.logical_not(is_task))
    def _():
        wait_for(send_b, b_send)
        wait_for(colf.at[pl.ds(0, 7), mine], e_send)


def comm_call(starts, sel, wf, s, t, q, z):
    dma = pltpu.SemaphoreType.DMA
    br, w, bc, _ = s.shape
    return pl.pallas_call(
        comm_kernel,
        out_shape=[
            pltpu.VMEM((br, W, W), F32), pltpu.VMEM((4, bc, br * w, w), F32),
        ],
        in_specs=[pl.BlockSpec(memory_space=pltpu.HBM)] * 7,
        out_specs=[VM, VM],
        scratch_shapes=[
            pltpu.VMEM((NT, W, W), F32), pltpu.VMEM((NT, W, W), BF), pltpu.VMEM((NT, W, W), BF),
            pltpu.VMEM(starts.shape, jnp.int32), pltpu.VMEM(sel.shape, jnp.int32),
            pltpu.VMEM((NK, 2, W, W), F32), pltpu.VMEM((NQ, 2, NK, 8, 128), F32),
            pltpu.VMEM((8, 128), jnp.int32), pltpu.SMEM((8, 128), jnp.int32),
            pltpu.VMEM((17, NK, 8, 128), F32), pltpu.VMEM((32, NK, 8, 128), F32),
            pltpu.VMEM((NK, W, W), F32), pltpu.VMEM((W, W), F32), pltpu.VMEM((4, br, w, bc, w), F32),
            pltpu.SemaphoreType.REGULAR, dma((2,)), dma, dma, dma((4,)), dma, dma, dma, dma, dma,
            dma, dma, dma, dma((15, SUB)), dma, dma, dma, dma, dma((2, 2, DSUB)),
        ],
        compiler_params=pltpu.CompilerParams(has_side_effects=True, vmem_limit_bytes=24 * 1024 * 1024, collective_id=0),
        name="comm",
    )(*(pltpu.with_memory_space_constraint(v, pltpu.HBM) for v in (starts, sel, wf, s, t, q, z)))


def finish_kernel(xs, rowl, os, ot, oq, oz, obuf, rh, rl, out_sem):
    _, bc, rows, w = xs.shape
    br = rows // w
    outs = (os, ot, oq, oz)

    def store(src, m, a, b):
        pltpu.make_async_copy(src.at[m, b, pl.ds(a * w, w)], outs[m].at[a, :, b, :], out_sem).start()

    for b in range(bc):
        for m in range(2, 4):
            for a in range(br):
                store(xs, m, a, b)
    for a in range(br):
        rh[a], rl[a] = split(rowl[a].T)

    def row_blocks(b, _):
        for m in range(2):
            for a in range(br):
                part = pl.ds(a * w, w)
                obuf[m, b, part] = mm((rh[a], rl[a]), split(xs[m, b, part]))
        for m in range(2):
            for a in range(br):
                store(obuf, m, a, b)
        return 0

    lax.fori_loop(0, bc, row_blocks, 0)
    pltpu.make_async_copy(xs, xs, out_sem).wait()


def finish_call(shape, xs, rowl):
    br, w, bc, _ = shape
    return pl.pallas_call(
        finish_kernel,
        out_shape=[jax.ShapeDtypeStruct(shape, F32)] * 4,
        in_specs=[VM, VM],
        out_specs=[ANY] * 4,
        scratch_shapes=[
            pltpu.VMEM((2,) + xs.shape[1:], F32),
            pltpu.VMEM((br, w, w), BF), pltpu.VMEM((br, w, w), BF),
            pltpu.SemaphoreType.DMA,
        ],
        compiler_params=pltpu.CompilerParams(vmem_limit_bytes=24 * 1024 * 1024),
        name="finish",
    )(xs, rowl)


def shards(s, t, q, z, starts, sel, wf):
    rowl, xs = comm_call(starts, sel, wf, s, t, q, z)
    return finish_call(s.shape, xs, rowl)


def solution(mesh):
    spec = P(None, "row", None, "col")
    return jax.shard_map(
        shards,
        mesh=mesh,
        in_specs=(spec,) * 4 + (P(), P(), P(None, "row")),
        out_specs=(spec,) * 4,
        check_vma=False,
    )
```

```python
import functools

import jax
import jax.numpy as jnp
from jax import lax
from jax.experimental import pallas as pl
from jax.experimental.pallas import tpu as pltpu
from jax.sharding import PartitionSpec as P

F32, BF = jnp.float32, jnp.bfloat16
MESH = pl.DeviceIdType.MESH
ANY = pl.BlockSpec(memory_space=pl.ANY)
VM = pl.BlockSpec(memory_space=pltpu.VMEM)
W = 256
NQ, NC, NB, NK = 8, 8, 4, 3


def div(a, b):
    return lax.div(a, jnp.int32(b))


def rem(a, b):
    return lax.rem(a, jnp.int32(b))


def split(x):
    hi = x.astype(BF)
    return hi, (x - hi.astype(F32)).astype(BF)


def mm(a, b):
    d = functools.partial(jnp.dot, preferred_element_type=F32)
    return d(a[0], b[0]) + (d(a[0], b[1]) + d(a[1], b[0]))

NT = 2 * NB
SUB, DSUB = 2, 4


def permute_rows(sel, wf, send, r, c):
    lane = lax.broadcasted_iota(jnp.int32, (32, W), 1)
    pos = lax.broadcasted_iota(jnp.int32, (32, W), 0) + c * 32
    pos1 = lax.broadcasted_iota(jnp.int32, (32, 1), 0) + c * 32
    for k in range(NK):
        flags = jnp.broadcast_to(sel[k, pl.ds(r, 1), :], (32, W))
        earlier = jnp.sum(jnp.where(lane < pos, flags, 0), axis=1, keepdims=True)
        own = jnp.sum(jnp.where(lane == pos, flags, 0), axis=1, keepdims=True)
        chosen = jnp.sum(flags, axis=1, keepdims=True)
        target = jnp.where(own == 1, earlier, chosen + pos1 - earlier)
        onehot = jnp.where(lane == target, 1.0, 0.0).astype(BF)
        for x in range(2):
            f = wf[k, x]
            hi = f.astype(BF)
            rest = f - hi.astype(F32)
            mid = rest.astype(BF)
            lo = (rest - mid.astype(F32)).astype(BF)
            d = functools.partial(jnp.dot, preferred_element_type=F32)
            rows = (d(onehot, hi) + d(onehot, mid)) + d(onehot, lo)
            for q in range(NQ):
                send[q, x, k] = rows[(q // 2) * 8:(q // 2) * 8 + 8, (q % 2) * 128:(q % 2) * 128 + 128]


def window_of_block(starts, inv):
    win = lax.broadcasted_iota(jnp.int32, (16, 16), 0)
    win_l = lax.broadcasted_iota(jnp.int32, (16, 16), 1)
    blk = lax.broadcasted_iota(jnp.int32, (16, 128), 1)
    win_b = lax.broadcasted_iota(jnp.int32, (16, 128), 0)
    for k in range(NK):
        st = jnp.broadcast_to(starts[k:k + 1, :], (16, 16))
        col = jnp.sum(jnp.where(win == win_l, st, 0), axis=1, keepdims=True)
        inv[k:k + 1, :] = 16 - jnp.max(jnp.where(col == blk, 16 - win_b, 0), axis=0, keepdims=True)


def task_chip(b, x, c):
    b, c = jnp.int32(b), jnp.int32(c)
    xx = rem(div(c, 4) + x + 2 * rem(b, 2), 4)
    y = rem(div(b, 2) + (1 - x) * rem(div(c, 2), 2), 2)
    return xx * 2 + y


def task_of(xx, y, c):
    bx = rem(xx + 4 - div(c, 4), 4)
    kind = rem(bx, 2)
    return kind, div(bx, 2) + 2 * rem(y + (1 - kind) * rem(div(c, 2), 2), 2)


def comm_kernel(starts_in, sel_in, wf, s_in, t_in, q_in, z_in, rowl, xs, colf, ch, cl,
                starts, sel, wf_v, send_a, inv_v, inv, recv_a, send_b, recv_b, combo, raw,
                ready, s_sem, w_sem, i_sem, raw_sem, x_sem, a_send, a_recv, b_send, b_recv,
                o_send, o_recv, c_send, c_recv, e_send, e_recv, t_send, d_send, d_recv):
    r, c = lax.axis_index("row"), lax.axis_index("col")
    x, y, h = div(r, 4), rem(div(r, 2), 2), rem(r, 2)
    q, z = div(r, 2), div(c, 2)
    rt, lt = c * 4 + div(q, 2), rem(q, 2)
    kind, task_b = task_of(x, y, c)
    is_task = kind == h

    barrier = pltpu.get_barrier_semaphore()

    def signal(sem, rr, cc):
        pl.semaphore_signal(sem, inc=1, device_id=(rr, cc), device_id_type=MESH)

    load_i = [pltpu.make_async_copy(starts_in, starts, s_sem.at[0]), pltpu.make_async_copy(sel_in, sel, s_sem.at[1])]
    for copy in load_i:
        copy.start()
    load_w = pltpu.make_async_copy(wf.at[:, 0], wf_v, w_sem)
    load_w.start()
    for i in (4, 5, 3, 2, 6, 1, 7):
        signal(barrier, r, rem(c + i, NC))
    for i in range(1, 16):
        signal(barrier, rem(r + i, 16), c)

    def remote(src, dst, ssem, rsem, rr, cc):
        pltpu.make_async_remote_copy(src, dst, ssem, rsem, device_id=(rr, cc), device_id_type=MESH).start()

    def put(src, dst, ssem, rsem, rr, cc):
        me = jnp.logical_and(rr == r, cc == c)

        @pl.when(me)
        def _():
            pltpu.make_async_copy(src, dst, rsem).start()

        @pl.when(jnp.logical_not(me))
        def _():
            remote(src, dst, ssem, rsem, rr, cc)

    def wait_for(ref, sem):
        pltpu.make_async_copy(ref, ref, sem).wait()

    load_x = [pltpu.make_async_copy(m, raw.at[i], raw_sem.at[i]) for i, m in enumerate((s_in, t_in, q_in, z_in))]
    for copy in load_x:
        copy.start()
    for copy in load_i:
        copy.wait()
    window_of_block(starts, inv_v)
    ident = jnp.where(
        lax.broadcasted_iota(jnp.int32, (8, 128), 0) + rt * 8
        == lax.broadcasted_iota(jnp.int32, (8, 128), 1) + lt * 128, 1.0, 0.0).astype(F32)
    for k in range(NK):
        recv_a[16, k] = ident
    load_w.wait()
    permute_rows(sel, wf_v, send_a, r, c)
    move_inv = pltpu.make_async_copy(inv_v, inv, i_sem)
    move_inv.start()

    pl.semaphore_wait(barrier, 15 + NC - 1)

    for i in range(1, 16):
        rr = rem(r + i, 16)
        remote(send_a.at[div(rr, 2), rem(rr, 2)], recv_a.at[r], a_send, a_recv, rr, c)
    pltpu.make_async_copy(send_a.at[q, h], recv_a.at[r], a_recv).start()
    for i in (4, 5, 3, 2, 6, 1, 7):
        signal(ready, r, rem(c + i, NC))
    move_inv.wait()
    pl.semaphore_wait(ready, NC - 1)
    wait_for(recv_a.at[pl.ds(0, 16)], a_recv)

    place = recv_b.at[:, pl.ds(pl.multiple_of(rt * 8, 8), 8), pl.ds(pl.multiple_of(lt * 128, 128), 128)]
    for i in range(32):
        for k in range(NK):
            send_b[i, k] = recv_a[inv[k, i], k]
    for i in (4, 5, 3, 2, 6, 1, 7):
        cc = rem(c + i, NC)
        for b in range(NB):
            remote(send_b.at[cc + NC * b], place, b_send, b_recv, task_chip(b, h, cc) * 2 + h, cc)
    for i in range(1, NB):
        b = rem(task_b + i, NB)
        remote(send_b.at[c + NC * b], place, b_send, b_recv, task_chip(b, h, c) * 2 + h, c)
    put(send_b.at[c + NC * task_b], place, b_send, b_recv, task_chip(task_b, h, c) * 2 + h, c)

    for copy in load_x:
        copy.wait()
    for i in range(4):
        for a in range(2):
            for b in range(NB):
                pltpu.make_async_copy(raw.at[i, a, :, b, :], xs.at[i, b, pl.ds(a * W, W)], x_sem).start()

    def part(first, count):
        return pl.ds(pl.multiple_of(first, 8), count)

    mine, theirs = part(h * 128, 128), part((1 - h) * 128, 128)
    near, far = 0, 1

    def piece(side, u):
        return part(h * 128 + side * 64 + u * (64 // SUB), 64 // SUB)

    partner = r + 1 - 2 * h

    def slot_at(dx, dy):
        kk, bb = task_of(rem(x + dx, 4), rem(y + dy, 2), c)
        return kk * NB + bb

    def row_piece(p, u):
        return pl.ds(p * 128 + u * (128 // DSUB), 128 // DSUB)

    own = kind * NB + task_b

    @pl.when(is_task)
    def _():
        wait_for(recv_b, b_recv)
        combo[...] = mm(split(mm(split(recv_b[0]), split(recv_b[1]))), split(recv_b[2]))
        @pl.when(kind == 0)
        def _():
            for u in range(DSUB):
                for p in range(2):
                    rows = row_piece(p, u)
                    land, arrived = rowl.at[div(task_b, 2), rows], d_recv.at[div(task_b, 2), p, u]
                    put(combo.at[rows], land, t_send, arrived, c + NC * rem(task_b, 2), c)
                    remote(combo.at[rows], land, t_send, arrived, c + NC * rem(task_b, 2), c + 1 - 2 * rem(c, 2))

        pltpu.make_async_copy(combo.at[mine], colf.at[own, mine], o_recv).start()
        remote(combo.at[theirs], colf.at[own, theirs], o_send, o_recv, partner, c)
        pltpu.make_async_copy(combo.at[theirs], colf.at[own, theirs], e_recv).start()

    left, right = rem(r + 12, 16), rem(r + 4, 16)
    across = x * 4 + (1 - y) * 2 + h

    def got(slot, side, i):
        for u in range(SUB):
            wait_for(colf.at[slot, piece(side, u)], c_recv.at[i, u])

    def send_piece(slot, side, u, i, rr):
        rows = piece(side, u)
        remote(colf.at[slot, rows], colf.at[slot, rows], c_send, c_recv.at[i, u], rr, c)

    def relay(slot, side, i, *hops):
        for u in range(SUB):
            wait_for(colf.at[slot, piece(side, u)], c_recv.at[i, u])
            for j, rr in hops:
                send_piece(slot, side, u, j, rr)

    def share(slot):
        remote(colf.at[slot, mine], colf.at[slot, mine], e_send, e_recv, partner, c)

    zd = rem(z + 4 - div(rem(r, NC), 2), 4)

    def got_row(a, p):
        for u in range(DSUB):
            wait_for(rowl.at[a, row_piece(p, u)], d_recv.at[a, p, u])

    def relay_rows(*sides):
        for u in range(DSUB):
            for a in range(2):
                for p in sides:
                    rows = row_piece(p, u)
                    wait_for(rowl.at[a, rows], d_recv.at[a, p, u])
                    remote(rowl.at[a, rows], rowl.at[a, rows], d_send, d_recv.at[a, p, u],
                           r, rem(c + (2 if p == 0 else NC - 2), NC))

    wait_for(colf.at[own, mine], o_recv)
    for u in range(SUB):
        send_piece(own, near, u, 1, right)
        send_piece(own, far, u, 4, left)
        send_piece(own, near, u, 5, across)
    for u in range(SUB):
        send_piece(own, far, u, 6, across)
        send_piece(own, far, u, 2, right)
        send_piece(own, near, u, 3, left)

    @pl.when(is_task)
    def _():
        share(own)

    @pl.when(zd == 0)
    def _():
        relay_rows(0, 1)

    at_left, at_right, at_across = slot_at(3, 0), slot_at(1, 0), slot_at(0, 1)
    relay(at_left, near, 1, (7, right), (9, across))
    relay(at_right, far, 4, (8, left), (12, across))
    relay(at_across, near, 5, (11, left))
    relay(at_across, far, 6, (10, right))
    share(at_across)

    @pl.when(zd == 1)
    def _():
        relay_rows(0)

    @pl.when(zd == 3)
    def _():
        relay_rows(1)

    got(at_left, far, 2)
    share(at_left)
    got(at_right, near, 3)
    share(at_right)
    across_left, across_right = slot_at(3, 1), slot_at(1, 1)
    relay(across_left, near, 9, (13, right))
    relay(across_right, far, 12, (14, left))

    @pl.when(zd == 2)
    def _():
        relay_rows(0, 1)

    got(across_left, far, 10)
    share(across_left)
    got(across_right, near, 11)
    share(across_right)
    opposite, across_opposite = slot_at(2, 0), slot_at(2, 1)
    got(opposite, near, 7)
    got(opposite, far, 8)
    share(opposite)
    got(across_opposite, near, 13)
    got(across_opposite, far, 14)
    share(across_opposite)

    wait_for(xs, x_sem)
    wait_for(recv_a.at[pl.ds(0, 15)], a_send)
    wait_for(colf.at[:, theirs], e_recv)

    def halves(i, _):
        ch[i], cl[i] = split(colf[i])
        return 0

    def columns(b, _):
        for m in range(4):
            f = b if m == 2 else NB + b
            xs[m, b] = mm(split(xs[m, b]), (ch[f], cl[f]))
        return 0

    lax.fori_loop(0, NT, halves, 0)
    lax.fori_loop(0, NB, columns, 0)
    wait_for(colf.at[pl.ds(0, 7), mine], c_send)

    @pl.when(zd == 1)
    def _():
        got_row(0, 1)
        got_row(1, 1)

    @pl.when(zd == 3)
    def _():
        got_row(0, 0)
        got_row(1, 0)

    @pl.when(zd % 2 == 0)
    def _():
        wait_for(rowl, d_send)

    @pl.when(zd % 2 == 1)
    def _():
        wait_for(rowl.at[0], d_send)

    @pl.when(is_task)
    def _():
        wait_for(send_b.at[pl.ds(0, 31)], b_send)
        wait_for(combo.at[theirs], o_send)
        wait_for(colf.at[:, mine], e_send)

        @pl.when(kind == 0)
        def _():
            local = c + NC * (rem(task_b, 2)) == r

            @pl.when(local)
            def _():
                wait_for(rowl.at[0], t_send)

            @pl.when(jnp.logical_not(local))
            def _():
                wait_for(rowl, t_send)

    @pl.when(jnp.logical_not(is_task))
    def _():
        wait_for(send_b, b_send)
        wait_for(colf.at[pl.ds(0, 7), mine], e_send)


def comm_call(starts, sel, wf, s, t, q, z):
    dma = pltpu.SemaphoreType.DMA
    br, w, bc, _ = s.shape
    return pl.pallas_call(
        comm_kernel,
        out_shape=[
            pltpu.VMEM((br, W, W), F32), pltpu.VMEM((4, bc, br * w, w), F32),
        ],
        in_specs=[pl.BlockSpec(memory_space=pltpu.HBM)] * 7,
        out_specs=[VM, VM],
        scratch_shapes=[
            pltpu.VMEM((NT, W, W), F32), pltpu.VMEM((NT, W, W), BF), pltpu.VMEM((NT, W, W), BF),
            pltpu.VMEM(starts.shape, jnp.int32), pltpu.VMEM(sel.shape, jnp.int32),
            pltpu.VMEM((NK, 2, W, W), F32), pltpu.VMEM((NQ, 2, NK, 8, 128), F32),
            pltpu.VMEM((8, 128), jnp.int32), pltpu.SMEM((8, 128), jnp.int32),
            pltpu.VMEM((17, NK, 8, 128), F32), pltpu.VMEM((32, NK, 8, 128), F32),
            pltpu.VMEM((NK, W, W), F32), pltpu.VMEM((W, W), F32), pltpu.VMEM((4, br, w, bc, w), F32),
            pltpu.SemaphoreType.REGULAR, dma((2,)), dma, dma, dma((4,)), dma, dma, dma, dma, dma,
            dma, dma, dma, dma((15, SUB)), dma, dma, dma, dma, dma((2, 2, DSUB)),
        ],
        compiler_params=pltpu.CompilerParams(has_side_effects=True, vmem_limit_bytes=24 * 1024 * 1024, collective_id=0),
        name="comm",
    )(*(pltpu.with_memory_space_constraint(v, pltpu.HBM) for v in (starts, sel, wf, s, t, q, z)))


def finish_kernel(xs, rowl, os, ot, oq, oz, obuf, rh, rl, out_sem):
    _, bc, rows, w = xs.shape
    br = rows // w
    outs = (os, ot, oq, oz)

    def store(src, m, a, b):
        pltpu.make_async_copy(src.at[m, b, pl.ds(a * w, w)], outs[m].at[a, :, b, :], out_sem).start()

    for b in range(bc):
        for m in range(2, 4):
            for a in range(br):
                store(xs, m, a, b)
    for a in range(br):
        rh[a], rl[a] = split(rowl[a].T)

    def row_blocks(b, _):
        for m in range(2):
            for a in range(br):
                part = pl.ds(a * w, w)
                obuf[m, b, part] = mm((rh[a], rl[a]), split(xs[m, b, part]))
        for m in range(2):
            for a in range(br):
                store(obuf, m, a, b)
        return 0

    lax.fori_loop(0, bc, row_blocks, 0)
    pltpu.make_async_copy(xs, xs, out_sem).wait()


def finish_call(shape, xs, rowl):
    br, w, bc, _ = shape
    return pl.pallas_call(
        finish_kernel,
        out_shape=[jax.ShapeDtypeStruct(shape, F32)] * 4,
        in_specs=[VM, VM],
        out_specs=[ANY] * 4,
        scratch_shapes=[
            pltpu.VMEM((2,) + xs.shape[1:], F32),
            pltpu.VMEM((br, w, w), BF), pltpu.VMEM((br, w, w), BF),
            pltpu.SemaphoreType.DMA,
        ],
        compiler_params=pltpu.CompilerParams(vmem_limit_bytes=24 * 1024 * 1024),
        name="finish",
    )(xs, rowl)


def shards(s, t, q, z, starts, sel, wf):
    rowl, xs = comm_call(starts, sel, wf, s, t, q, z)
    return finish_call(s.shape, xs, rowl)


def solution(mesh):
    spec = P(None, "row", None, "col")
    return jax.shard_map(
        shards,
        mesh=mesh,
        in_specs=(spec,) * 4 + (P(), P(), P(None, "row")),
        out_specs=(spec,) * 4,
        check_vma=False,
    )
```
